256 devices in a mesh: dp: 2 (over core), seq: 16 (over z, x_lo), mp: 8 (over x_hi, y).
Axes of the slice: x: 4 (x_hi: 2, x_lo: 2; x = x_hi * 2 + x_lo), y: 4, z: 8, core: 2. Of those that a mesh axis runs over, the one named last changes fastest.
Arguments:
- queries: bfloat16 [4, 2048, 4096], P('dp', 'seq', 'mp'), may hold values from -6 to 6
- vision: bfloat16 [4, 1280, 4096], P('dp', 'seq'), may hold values from -6 to 6
- key_weight: bfloat16 [4096, 1024], P(None, 'mp'), may hold values from -0.09375 to 0.09375
- value_weight: bfloat16 [4096, 1024], P(None, 'mp'), may hold values from -0.09375 to 0.09375
- query_gain: float32 [128], replicated, may hold values from 0.6 to 6
- key_gain: float32 [128], replicated, may hold values from 0.6 to 6
- out_grad: bfloat16 [4, 2048, 4096], P('dp', 'seq', 'mp'), may hold values from -6 to 6
- tile_count: int32 [4], P('dp'), may hold values from 1 to 4, as said below
Outputs:
- query_grad: bfloat16 [4, 2048, 4096], P('dp', 'seq', 'mp')
- vision_grad: bfloat16 [4, 1280, 4096], P('dp', 'seq', 'mp')
- key_weight_grad: float32 [4096, 1024], P(None, 'mp')
- value_weight_grad: float32 [4096, 1024], P(None, 'mp')
The draws below stay inside these ranges and needn't reach their ends.
Inputs may be any that keep to these rules, and one draw needn't show every extreme that they name: The live vision tokens of sample s are its first tile_count[s] * 320; some sample has 4 tiles and some other sample has 1.
All inputs are finite; a program needn't handle non-finite values.
Results may differ from the reference program's by a relative error of at most 0.03.
The reference program's roundings to bfloat16 on the way (of `keys`, `values`, `normed`, `probs_b`, `attn`, `dscores`, `key_grad` and `value_grad`) count: a program that leaves them out, or rounds other values in their place, can miss the bound.
Values may be sent and summed in bfloat16 or wider, within the bound.
A program may use at most 64 MiB of HBM per device.

```python
import jax
import jax.numpy as jnp
from jax import lax

D = 4096
HEADS = 32
KV_HEADS = 8
HEAD_DIM = 128
MAX_TILES = 4
SAMPLES = 4
TXT = 2048
VIS = 1280
TILE_TOK = 320


def vision_field(key):
    drawn = jax.random.normal(jax.random.fold_in(key, 7001), (SAMPLES, VIS, D), jnp.float32)
    return jnp.clip(drawn, -6.0, 6.0)


def key_matrix(key):
    drawn = jax.random.normal(jax.random.fold_in(key, 7002), (D, KV_HEADS * HEAD_DIM), jnp.float32)
    return jnp.clip(drawn, -6.0, 6.0) * D ** (-0.5)


def draw_vision(key, part):
    return vision_field(key).astype(jnp.bfloat16)


def draw_key_weight(key, part):
    return key_matrix(key).astype(jnp.bfloat16)


def draw_queries(key, part):
    drawn = jax.random.normal(jax.random.fold_in(key, 7003), (SAMPLES, TXT, HEADS * HEAD_DIM), jnp.float32)
    drawn = jnp.clip(drawn, -6.0, 6.0)
    return drawn.astype(jnp.bfloat16)


def draw_query_gain(key, part):
    inner = jax.random.fold_in(key, 7005)
    return jax.random.uniform(inner, (HEAD_DIM,), jnp.float32, 0.6, 1.4)


def draw_key_gain(key, part):
    inner = jax.random.fold_in(key, 7006)
    return jax.random.uniform(inner, (HEAD_DIM,), jnp.float32, 0.6, 1.4)


def draw_tile_count(key, part):
    counts = jax.random.randint(jax.random.fold_in(key, 7101), (SAMPLES,), 1, MAX_TILES + 1, dtype=jnp.int32)
    full_at = jax.random.randint(jax.random.fold_in(key, 7102), (), 0, SAMPLES, dtype=jnp.int32)
    step_to = jax.random.randint(jax.random.fold_in(key, 7103), (), 1, SAMPLES, dtype=jnp.int32)
    single_at = (full_at + step_to) % SAMPLES
    counts = counts.at[full_at].set(MAX_TILES)
    counts = counts.at[single_at].set(1)
    return counts.astype(jnp.int32)


def steps_of(stream_key, extent, pieces, smallest, top_value):
    def one(dim, shards_of):
        heights = jax.random.uniform(jax.random.fold_in(jax.random.fold_in(stream_key, 6), dim), (shards_of,), jnp.float32, smallest / len(pieces), top_value / len(pieces))
        return jnp.repeat(jnp.exp(heights), extent[dim] // shards_of).reshape((-1,) + (1,) * (len(extent) - dim - 1))

    level = one(*pieces[0])
    for cut in pieces[1:]:
        level = level * one(*cut)
    return level


def noise(own_key, dims, scale, bound, split=(), kind=jnp.bfloat16):
    values = jax.random.normal(own_key, dims, jnp.float32) * scale
    if len(split) > 0:
        values = steps_of(own_key, dims, split, -0.22, 0.18) * values
    return jnp.clip(values, min=-bound, max=bound).astype(kind)


def setup_inputs(seed: int = 0) -> dict:
    key_of = jax.random.split(jax.random.key(seed), 9)
    queries = draw_queries(jax.random.fold_in(key_of[8], 71), 0)
    vision = draw_vision(jax.random.fold_in(key_of[8], 71), 0)
    key_weight = draw_key_weight(jax.random.fold_in(key_of[8], 71), 0)
    value_weight = noise(key_of[3], (D, KV_HEADS * HEAD_DIM), D ** -0.5, 0.09375, ((1, 8),))
    query_gain = draw_query_gain(jax.random.fold_in(key_of[8], 71), 0)
    key_gain = draw_key_gain(jax.random.fold_in(key_of[8], 71), 0)
    out_grad = noise(key_of[6], (SAMPLES, TXT, HEADS * HEAD_DIM), 1.0, 6.0, ((0, 2), (1, 16), (2, 8)))
    tile_count = draw_tile_count(jax.random.fold_in(key_of[8], 71), 0)
    return {"queries": queries, "vision": vision, "key_weight": key_weight, "value_weight": value_weight, "query_gain": query_gain, "key_gain": key_gain, "out_grad": out_grad, "tile_count": tile_count}


EPS = 1e-05
NEG = -1e+30

def norm_apply(raw, gain):
    inverse = lax.rsqrt(lax.optimization_barrier(jnp.mean(raw * raw, axis=-1, keepdims=True)) + EPS)
    return (raw * inverse * gain, inverse)

def norm_back(raw, inverse, gain, upstream):
    weighted = upstream * gain
    return inverse * weighted - raw * inverse * inverse * inverse * lax.optimization_barrier(jnp.mean(weighted * raw, axis=-1, keepdims=True))

def sample_grads(queries_one, vision_one, out_one, tiles_one, key_weight, value_weight, query_gain, key_gain):
    group_size = HEADS // KV_HEADS
    score_scale = HEAD_DIM ** (-0.5)
    key_cols = key_weight.reshape(D, KV_HEADS, HEAD_DIM).transpose(1, 0, 2)
    value_cols = value_weight.reshape(D, KV_HEADS, HEAD_DIM).transpose(1, 0, 2)
    query_heads = queries_one.reshape(TXT, KV_HEADS, group_size, HEAD_DIM).transpose(1, 0, 2, 3)
    out_heads = out_one.reshape(TXT, KV_HEADS, group_size, HEAD_DIM).transpose(1, 0, 2, 3)
    live_keys = jnp.arange(VIS, dtype=jnp.int32) < tiles_one * TILE_TOK

    def one_group(vision_total, inputs):
        key_col, value_col, query_group, out_group = inputs
        key_raw = jnp.dot(vision_one, key_col, preferred_element_type=jnp.float32)
        key_normed, key_inverse = norm_apply(key_raw, key_gain)
        keys = key_normed.astype(jnp.bfloat16)
        values = jnp.dot(vision_one, value_col, preferred_element_type=jnp.float32).astype(jnp.bfloat16)
        query_raw = query_group.astype(jnp.float32)
        query_normed, query_inverse = norm_apply(query_raw, query_gain)
        normed = query_normed.astype(jnp.bfloat16)
        normed_wide = normed.astype(jnp.float32)
        keys_wide = keys.astype(jnp.float32)
        values_wide = values.astype(jnp.float32)
        out_wide = out_group.astype(jnp.float32)
        scores = jnp.einsum('tgd,jd->gtj', normed_wide, keys_wide) * score_scale
        scores = jnp.where(live_keys[None, None, :], scores, NEG)
        row_top = lax.optimization_barrier(jnp.max(scores, axis=-1, keepdims=True))
        expo = jnp.exp(scores - row_top)
        probs = expo / lax.optimization_barrier(jnp.sum(expo, axis=-1, keepdims=True))
        probs_b = probs.astype(jnp.bfloat16)
        probs_wide = probs_b.astype(jnp.float32)
        attn = jnp.einsum('gtj,jd->tgd', probs_wide, values_wide).astype(jnp.bfloat16)
        delta = lax.optimization_barrier(jnp.sum(out_wide * attn.astype(jnp.float32), axis=-1))
        dprobs = jnp.einsum('tgd,jd->gtj', out_wide, values_wide)
        dscores = (probs * (dprobs - delta.T[:, :, None])).astype(jnp.bfloat16)
        dscores_wide = dscores.astype(jnp.float32)
        dnormed = jnp.einsum('gtj,jd->tgd', dscores_wide, keys_wide) * score_scale
        dkeys = jnp.einsum('gtj,tgd->jd', dscores_wide, normed_wide) * score_scale
        dvalues = jnp.einsum('gtj,tgd->jd', probs_wide, out_wide)
        query_part = norm_back(query_raw, query_inverse, query_gain, dnormed).astype(jnp.bfloat16)
        key_grad = norm_back(key_raw, key_inverse, key_gain, dkeys).astype(jnp.bfloat16)
        value_grad = dvalues.astype(jnp.bfloat16)
        key_weight_part = jnp.dot(vision_one.T, key_grad, preferred_element_type=jnp.float32)
        value_weight_part = jnp.dot(vision_one.T, value_grad, preferred_element_type=jnp.float32)
        vision_term = jnp.dot(key_grad, key_col.T, preferred_element_type=jnp.float32)
        vision_term = vision_term + jnp.dot(value_grad, value_col.T, preferred_element_type=jnp.float32)
        return (vision_total + vision_term, (query_part, key_weight_part, value_weight_part))
    start_total = jnp.zeros((VIS, D), jnp.float32)
    vision_total, stacked = lax.scan(one_group, start_total, (key_cols, value_cols, query_heads, out_heads))
    query_parts, key_parts, value_parts = stacked
    query_grad = query_parts.transpose(1, 0, 2, 3).reshape(TXT, HEADS * HEAD_DIM)
    key_weight_part = key_parts.transpose(1, 0, 2).reshape(D, KV_HEADS * HEAD_DIM)
    value_weight_part = value_parts.transpose(1, 0, 2).reshape(D, KV_HEADS * HEAD_DIM)
    return (query_grad, vision_total.astype(jnp.bfloat16), key_weight_part, value_weight_part)

def reference(queries, vision, key_weight, value_weight, query_gain, key_gain, out_grad, tile_count):
    query_list = []
    vision_list = []
    key_weight_grad = jnp.zeros((D, KV_HEADS * HEAD_DIM), jnp.float32)
    value_weight_grad = jnp.zeros((D, KV_HEADS * HEAD_DIM), jnp.float32)
    for sample_at in range(SAMPLES):
        query_part, vision_part, key_part, value_part = sample_grads(queries[sample_at], vision[sample_at], out_grad[sample_at], tile_count[sample_at], key_weight, value_weight, query_gain, key_gain)
        query_list.append(query_part)
        vision_list.append(vision_part)
        key_weight_grad = key_weight_grad + key_part
        value_weight_grad = value_weight_grad + value_part
    return (jnp.stack(query_list), jnp.stack(vision_list), key_weight_grad, value_weight_grad)
```

```python
import functools

import jax
import jax.numpy as jnp
from jax import lax
from jax.experimental import pallas as pl
from jax.experimental.pallas import tpu as pltpu
from jax.sharding import PartitionSpec as P

EPS = 1e-05
NEG = -1e30
LOG2E = 1.4426950408889634
MESH = pl.DeviceIdType.MESH
NT = (((1,), (1,)), ((), ()))
TN = (((0,), (0,)), ((), ()))
F32 = jnp.float32
BF16 = jnp.bfloat16
N_COPY = 300

SEQ_A = ((0, 1, 4), (0, -1, 3), (1, 1, 3), (1, -1, 4))
SEQ_B = ((0, 1, 4), (0, -1, 3))
MP_A = ((0, 1, 2), (0, -1, 1), (1, 1, 1), (1, -1, 2))


def dot(a, b, dims=None):
    if dims is None:
        return jnp.dot(a, b, preferred_element_type=F32)
    return lax.dot_general(a, b, dims, preferred_element_type=F32)


class Copies:
    def __init__(self, send_sems, recv_sems):
        self.send_sems, self.recv_sems, self.all = send_sems, recv_sems, []

    def start(self, src, dst, device):
        at = len(self.all)
        copy = pltpu.make_async_remote_copy(
            src_ref=src,
            dst_ref=dst,
            send_sem=self.send_sems.at[at],
            recv_sem=self.recv_sems.at[at],
            device_id=device,
            device_id_type=MESH,
        )
        copy.start()
        self.all.append(copy)
        return copy

    def drain(self):
        for copy in self.all:
            copy.wait_send()


class Slots:
    def __init__(self, copies, stage, land):
        self.copies, self.stage, self.land, self.used = copies, stage, land, 0

    def send(self, value, device):
        at = self.used
        self.used += 1
        self.stage[at] = value.astype(BF16)
        copy = self.copies.start(self.stage.at[at], self.land.at[at], device)
        return copy, at

    def take(self, pending):
        copy, at = pending
        copy.wait_recv()
        return self.land[at].astype(F32)


def gather_a(copies, chunk, ring, across, hook):
    side = copies.start(chunk(0, 0), chunk(0, 0), across)
    pend = {}
    for i in (0, 1):
        pend[i] = copies.start(chunk(0, 0), chunk(0, 0), ring[SEQ_A[i][1]])
    hook(0, 0)
    yield
    side.wait_recv()
    for i in (2, 3):
        pend[i] = copies.start(chunk(0, 1), chunk(0, 1), ring[SEQ_A[i][1]])
    hook(0, 1)
    yield
    for t in range(1, 5):
        for i, (col, way, hops) in enumerate(SEQ_A):
            if t <= hops:
                pend[i].wait_recv()
                here = chunk(-way * t, col)
                if t < hops:
                    pend[i] = copies.start(here, here, ring[way])
                hook(-way * t, col)
        yield


def gather_b(copies, chunk, ring, across, hook):
    pend = {}
    for i in (0, 1):
        pend[i] = copies.start(chunk(0, 0), chunk(0, 0), ring[SEQ_B[i][1]])
    sides = [(0, copies.start(chunk(0, 0), chunk(0, 0), across))]
    hook(0, 0)
    yield
    for t in range(1, 5):
        for i, (col, way, hops) in enumerate(SEQ_B):
            if t <= hops:
                pend[i].wait_recv()
                here = chunk(-way * t, col)
                if t < hops:
                    pend[i] = copies.start(here, here, ring[way])
                sides.append((-way * t, copies.start(here, here, across)))
                hook(-way * t, col)
        yield
    for at, side in sides:
        side.wait_recv()
        hook(at, 1)


def scatter_a(slots, own, ring, across, streams, finish):
    pend = {}
    most = max(hops for _, _, hops in streams)
    for t in range(most):
        for i, (col, way, hops) in enumerate(streams):
            if t < hops:
                value = own(way * (hops - t), col)
                if t > 0:
                    value = value + slots.take(pend[i])
                pend[i] = slots.send(value, ring[way])
        yield
    value = own(0, 1)
    for i in (2, 3):
        value = value + slots.take(pend[i])
    side = slots.send(value, across)
    yield
    value = own(0, 0)
    for i in (0, 1):
        value = value + slots.take(pend[i])
    finish(value + slots.take(side))


def scatter_b(slots, own, ring, across, finish):
    sides = {}
    for at in (4, -3, 3, -2, 2, -1, 1, 0):
        sides[at] = slots.send(own(at, 1), across)
    yield
    pend = {}
    for t in range(4):
        for i, (_, way, hops) in enumerate(SEQ_B):
            if t < hops:
                at = way * (hops - t)
                value = own(at, 0) + slots.take(sides[at])
                if t > 0:
                    value = value + slots.take(pend[i])
                pend[i] = slots.send(value, ring[way])
        yield
    value = own(0, 0) + slots.take(sides[0])
    for i in (0, 1):
        value = value + slots.take(pend[i])
    finish(value)


def step(generators):
    alive = []
    for generator in generators:
        try:
            next(generator)
            alive.append(generator)
        except StopIteration:
            pass
    return alive


def kernel(
    sizes,
    q_hbm, vis_hbm, wk_hbm, wv_hbm, qgain_ref, kgain_ref, do_hbm, tiles_ref,
    qgrad, vgrad, wgk, wgv,
    vis, visw, w, q2, do2, qn, dot_t, kraw, kall, vall, s_ref, dk, dv, ksum, vsum,
    kvg, kvgp, wgt, stage_d, land_d, stage_e, land_e, stage_c, land_c,
    send_sems, recv_sems, in_sems,
):
    nz, ny = sizes
    samples, rows, tile = 2, 80, 320
    n_seq = 2 * nz
    heads = 4
    text = q_hbm.shape[1]
    width = vis_hbm.shape[1]
    half = width // 2
    slab = half // n_seq
    share = vgrad.shape[1]
    head_dim = 128
    score_scale = head_dim ** (-0.5)

    core = lax.axis_index("dp")
    seq = lax.axis_index("seq")
    mp = lax.axis_index("mp")
    z, col = seq // 2, lax.rem(seq, 2)
    xh, y = mp // ny, lax.rem(mp, ny)
    sign = 1 - 2 * core

    def z_at(k):
        return lax.rem(z + sign * k + 2 * nz, nz)

    def y_at(k):
        return lax.rem(y + k + 2 * ny, ny)

    ring = {k: {"seq": z_at(k) * 2 + col} for k in (1, -1)}
    across = {"seq": z * 2 + 1 - col}
    partner = {"dp": 1 - core}
    y_ring = {k: {"mp": xh * ny + y_at(k)} for k in (1, -1)}
    y_across = {"mp": (1 - xh) * ny + y}
    peers = (ring[1], ring[-1], across, partner, y_ring[1], y_ring[-1], y_across)

    local = []

    def load(src, dst):
        copy = pltpu.make_async_copy(src, dst, in_sems.at[len(local)])
        copy.start()
        local.append(copy)
        return copy

    parts = 4
    piece = width // parts
    loads = []
    for p in range(parts):
        cols = pl.ds(p * piece, piece)
        loads.append(
            (
                load(vis_hbm.at[:, cols], vis.at[:, cols]),
                load(wk_hbm.at[cols, :], w.at[cols, pl.ds(0, 128)]),
                load(wv_hbm.at[cols, :], w.at[cols, pl.ds(128, 128)]),
            )
        )
    q_loads = []
    for a in range(samples):
        for h in range(heads):
            here = pl.ds(h * text, text)
            q_loads.append(load(q_hbm.at[a, :, pl.ds(h * 128, 128)], q2.at[a, here, :]))
            q_loads.append(load(do_hbm.at[a, :, pl.ds(h * 128, 128)], do2.at[a, here, :]))
    mine = pl.ds(pl.multiple_of(core * half, 128), half)
    theirs = pl.ds(pl.multiple_of((1 - core) * half, 128), half)
    own_half = load(vis_hbm.at[:, mine], visw.at[pl.ds(0, samples * rows), :])

    barrier = pltpu.get_barrier_semaphore()
    for peer in peers:
        pl.semaphore_signal(barrier, inc=1, device_id=peer, device_id_type=MESH)

    total = jnp.zeros((samples * rows, 256), F32)
    for p in range(parts):
        for copy in loads[p]:
            copy.wait()
        total = total + dot(vis[:, p * piece : (p + 1) * piece], w[p * piece : (p + 1) * piece, :])
    key_raw = total[:, :128]
    kraw[...] = key_raw
    key_inverse = lax.rsqrt(jnp.mean(key_raw * key_raw, axis=-1, keepdims=True) + EPS)
    keys = (key_raw * key_inverse * kgain_ref[...]).astype(BF16)
    values = total[:, 128:].astype(BF16)
    own_rows = pl.ds(pl.multiple_of(seq * rows, 16), rows)
    for a in range(samples):
        kall[a, own_rows, :] = keys[a * rows : (a + 1) * rows]
        vall[a, own_rows, :] = values[a * rows : (a + 1) * rows]

    pl.semaphore_wait(barrier, len(peers))
    copies = Copies(send_sems, recv_sems)

    def owner(k, other):
        return z_at(k) * 2 + (1 - col if other else col)

    def no_hook(k, other):
        del k, other

    def key_chunk(ref, a):
        def chunk(k, other):
            return ref.at[a, pl.ds(pl.multiple_of(owner(k, other) * rows, 16), rows), :]

        return chunk

    first = [
        gather_a(copies, key_chunk(kall, 0), ring, across, no_hook),
        gather_b(copies, key_chunk(vall, 0), ring, across, no_hook),
    ]
    second = [
        gather_a(copies, key_chunk(kall, 1), ring, across, no_hook),
        gather_b(copies, key_chunk(vall, 1), ring, across, no_hook),
    ]

    def prepare(a):
        raw = q2[a].astype(F32)
        inverse = lax.rsqrt(jnp.mean(raw * raw, axis=-1, keepdims=True) + EPS)
        qn[a] = (raw * inverse * qgain_ref[...]).astype(BF16)
        for h in range(heads):
            block = do2[a, pl.ds(h * text, text), :].astype(F32)
            dot_t[a, :, pl.ds(h * text, text)] = block.T

    first = step(first)
    second = step(second)
    vision_swap = copies.start(
        vis_hbm.at[:, theirs], visw.at[pl.ds(samples * rows, samples * rows), :], partner
    )
    for copy in q_loads:
        copy.wait()
    prepare(0)
    first = step(first)
    second = step(second)
    prepare(1)
    while first:
        first = step(first)
        second = step(second)

    n_rows = heads * text

    def scores_pass(a):
        def body(k, row_max):
            at = pl.ds(pl.multiple_of(k * tile, tile), tile)
            s = dot(kall[a, at, :], qn[a], NT)
            s = s + jnp.where(k < tiles_ref[a], 0.0, NEG)
            s_ref[at, :] = s
            return jnp.maximum(row_max, jnp.max(s, axis=0, keepdims=True))

        return lax.fori_loop(0, 4, body, jnp.full((1, n_rows), NEG, F32))

    def exp_pass(row_max):
        def body(k, row_sum):
            at = pl.ds(pl.multiple_of(k * tile, tile), tile)
            e = jnp.exp2((s_ref[at, :] - row_max) * (score_scale * LOG2E))
            s_ref[at, :] = e
            return row_sum + jnp.sum(e, axis=0, keepdims=True)

        return 1.0 / lax.fori_loop(0, 4, body, jnp.zeros((1, n_rows), F32))

    def value_pass(a, inverse_sum):
        def body(k, attn):
            at = pl.ds(pl.multiple_of(k * tile, tile), tile)
            probs_b = (s_ref[at, :] * inverse_sum).astype(BF16)
            dv[a, at, :] = dot(probs_b, do2[a])
            return attn + dot(vall[a, at, :], probs_b, TN)

        attn = lax.fori_loop(0, 4, body, jnp.zeros((head_dim, n_rows), F32))
        return jnp.sum(dot_t[a] * attn.astype(BF16).astype(F32), axis=0, keepdims=True)

    def key_pass(a, inverse_sum, delta):
        def body(k, dn):
            at = pl.ds(pl.multiple_of(k * tile, tile), tile)
            dprobs = dot(vall[a, at, :], do2[a], NT)
            ds = (s_ref[at, :] * inverse_sum * (dprobs - delta)).astype(BF16)
            dk[a, at, :] = dot(ds, qn[a]) * score_scale
            return dn + dot(kall[a, at, :], ds, TN)

        return lax.fori_loop(0, 4, body, jnp.zeros((head_dim, n_rows), F32))

    def query_pass(a, dn):
        for h in range(heads):
            here = slice(h * text, (h + 1) * text)
            raw = q2[a, here, :].astype(F32)
            inverse = lax.rsqrt(jnp.mean(raw * raw, axis=-1, keepdims=True) + EPS)
            u = (dn[:, here] * score_scale).T * qgain_ref[...]
            mean = jnp.mean(u * raw, axis=-1, keepdims=True)
            grad = inverse * u - raw * (inverse * inverse * inverse) * mean
            qgrad[a, :, pl.ds(h * 128, 128)] = grad.astype(BF16)

    def own_part(ref, a):
        def own(k, other):
            return ref[a, pl.ds(pl.multiple_of(owner(k, other) * rows, 16), rows), :]

        return own

    def own_sum(ref, a):
        def finish(value):
            ref[pl.ds(a * rows, rows), :] = value

        return finish

    slots_d = Slots(copies, stage_d, land_d)

    def value_scatter(a):
        return scatter_b(slots_d, own_part(dv, a), ring, across, own_sum(vsum, a))

    def key_scatter(a):
        return scatter_a(slots_d, own_part(dk, a), ring, across, SEQ_A, own_sum(ksum, a))

    row_max = scores_pass(0)
    second = step(second)
    inverse_sum = exp_pass(row_max)
    second = step(second)
    delta = value_pass(0, inverse_sum)
    while second:
        second = step(second)
    going = step([value_scatter(0)])
    dn = key_pass(0, inverse_sum, delta)
    going = step(going + [key_scatter(0)])
    query_pass(0, dn)
    row_max = scores_pass(1)
    going = step(going)
    inverse_sum = exp_pass(row_max)
    going = step(going)
    delta = value_pass(1, inverse_sum)
    going = step(going + [value_scatter(1)])
    dn = key_pass(1, inverse_sum, delta)
    going = step(going + [key_scatter(1)])
    query_pass(1, dn)
    while going:
        going = step(going)

    raw = kraw[...]
    inverse = lax.rsqrt(jnp.mean(raw * raw, axis=-1, keepdims=True) + EPS)
    u = ksum[...] * kgain_ref[...]
    mean = jnp.mean(u * raw, axis=-1, keepdims=True)
    kvg[:, :128] = (inverse * u - raw * (inverse * inverse * inverse) * mean).astype(BF16)
    kvg[:, 128:] = vsum[...].astype(BF16)
    swap = copies.start(kvg, kvgp, partner)

    def vision_part(k, other):
        at = (1 - xh if other else xh) * ny + y_at(k)
        block = w[pl.ds(pl.multiple_of(at * share, share), share), :]
        return dot(kvg[...], block, NT)

    def vision_done(value):
        vgrad[...] = value.astype(BF16)

    slots_c = Slots(copies, stage_c, land_c)
    vision = step([scatter_a(slots_c, vision_part, y_ring, y_across, MP_A, vision_done)])

    swap.wait_recv()
    own_half.wait()
    vision_swap.wait_recv()
    own_t = kvg[...].astype(F32).T.astype(BF16)
    their_t = kvgp[...].astype(F32).T.astype(BF16)
    n_own = samples * rows
    for i in range(n_seq // 2):
        lanes = slice(i * 2 * slab, (i + 1) * 2 * slab)
        block = dot(own_t, visw[:n_own, lanes]) + dot(their_t, visw[n_own:, lanes])
        wgt[2 * i] = block[:, :slab]
        wgt[2 * i + 1] = block[:, slab:]

    def own_weight(which):
        def own(k, other):
            return wgt[owner(k, other), pl.ds(which * 128, 128), :]

        return own

    def weight_chunk(ref):
        def chunk(k, other):
            start = pl.multiple_of(core * half + owner(k, other) * slab, slab)
            return ref.at[pl.ds(start, slab), :]

        return chunk

    def weight_done(ref):
        def finish(value):
            start = pl.multiple_of(core * half + seq * slab, slab)
            ref[pl.ds(start, slab), :] = value.T.astype(BF16)

        return finish

    slots_e = Slots(copies, stage_e, land_e)
    going = [
        scatter_b(slots_e, own_weight(1), ring, across, weight_done(wgv)),
        scatter_a(slots_e, own_weight(0), ring, across, SEQ_A, weight_done(wgk)),
    ]
    for _ in range(4):
        going = step(going)
    vision = step(vision)
    while going:
        going = step(going)

    handed = []

    def hand_on(ref):
        def hook(k, other):
            here = weight_chunk(ref)(k, other)
            handed.append(copies.start(here, here, partner))

        return hook

    going = [
        gather_a(copies, weight_chunk(wgk), ring, across, hand_on(wgk)),
        gather_b(copies, weight_chunk(wgv), ring, across, hand_on(wgv)),
    ]
    for _ in range(3):
        going = step(going)
    vision = step(vision)
    while going:
        going = step(going)
    while vision:
        vision = step(vision)
    for copy in handed:
        copy.wait_recv()
    copies.drain()


def local(nz, ny, queries, vision, key_weight, value_weight, query_gain, key_gain, out_grad, tile_count):
    samples, rows, width = vision.shape
    text = queries.shape[1]
    n_seq = 2 * nz
    n_own = samples * rows
    n_vis = rows * n_seq
    n_rows = 4 * text
    half = width // 2
    slab = half // n_seq
    share = width // (2 * ny)
    hbm = pl.BlockSpec(memory_space=pl.ANY)
    vmem = pl.BlockSpec(memory_space=pltpu.VMEM)
    smem = pl.BlockSpec(memory_space=pltpu.SMEM)
    query_grad, vision_grad, wgk, wgv = pl.pallas_call(
        functools.partial(kernel, (nz, ny)),
        out_shape=(
            jax.ShapeDtypeStruct(queries.shape, BF16),
            jax.ShapeDtypeStruct((n_own, share), BF16),
            jax.ShapeDtypeStruct((width, 128), BF16),
            jax.ShapeDtypeStruct((width, 128), BF16),
        ),
        in_specs=[hbm, hbm, hbm, hbm, vmem, vmem, hbm, smem],
        out_specs=(vmem, vmem, vmem, vmem),
        scratch_shapes=[
            pltpu.VMEM((n_own, width), BF16),
            pltpu.VMEM((2 * n_own, half), BF16),
            pltpu.VMEM((width, 256), BF16),
            pltpu.VMEM((samples, n_rows, 128), BF16),
            pltpu.VMEM((samples, n_rows, 128), BF16),
            pltpu.VMEM((samples, n_rows, 128), BF16),
            pltpu.VMEM((samples, 128, n_rows), F32),
            pltpu.VMEM((n_own, 128), F32),
            pltpu.VMEM((samples, n_vis, 128), BF16),
            pltpu.VMEM((samples, n_vis, 128), BF16),
            pltpu.VMEM((n_vis, n_rows), F32),
            pltpu.VMEM((samples, n_vis, 128), F32),
            pltpu.VMEM((samples, n_vis, 128), F32),
            pltpu.VMEM((n_own, 128), F32),
            pltpu.VMEM((n_own, 128), F32),
            pltpu.VMEM((n_own, 256), BF16),
            pltpu.VMEM((n_own, 256), BF16),
            pltpu.VMEM((n_seq, 256, slab), F32),
            pltpu.VMEM((60, rows, 128), BF16),
            pltpu.VMEM((60, rows, 128), BF16),
            pltpu.VMEM((30, 128, slab), BF16),
            pltpu.VMEM((30, 128, slab), BF16),
            pltpu.VMEM((7, n_own, share), BF16),
            pltpu.VMEM((7, n_own, share), BF16),
            pltpu.SemaphoreType.DMA((N_COPY,)),
            pltpu.SemaphoreType.DMA((N_COPY,)),
            pltpu.SemaphoreType.DMA((40,)),
        ],
        compiler_params=pltpu.CompilerParams(
            collective_id=0, has_side_effects=True, vmem_limit_bytes=60 * 1024 * 1024
        ),
    )(
        queries,
        vision.reshape(n_own, width),
        key_weight,
        value_weight,
        query_gain.reshape(1, 128),
        key_gain.reshape(1, 128),
        out_grad,
        tile_count,
    )
    return (
        query_grad,
        vision_grad.reshape(samples, rows, share),
        wgk.astype(F32),
        wgv.astype(F32),
    )


def solution(mesh):
    nz = mesh.shape["seq"] // 2
    ny = mesh.shape["mp"] // 2
    in_specs = (
        P("dp", "seq", "mp"),
        P("dp", "seq", None),
        P(None, "mp"),
        P(None, "mp"),
        P(),
        P(),
        P("dp", "seq", "mp"),
        P("dp"),
    )
    out_specs = (P("dp", "seq", "mp"), P("dp", "seq", "mp"), P(None, "mp"), P(None, "mp"))
    return jax.shard_map(
        functools.partial(local, nz, ny), mesh=mesh, in_specs=in_specs, out_specs=out_specs, check_vma=False
    )
```
